32 devices in a mesh: rep: 4 (over y, x), fsdp: 4 (over z), tp: 2 (over core).
Axes of the slice: x: 2, y: 2, z: 4, core: 2. Of those that a mesh axis runs over, the one named last changes fastest.
Arguments:
- hidden: bfloat16 [4096, 4096], P(('rep', 'fsdp')), may hold values from -6 to 6
- norm_gain: float32 [4096], P('fsdp'), may hold values from 0.5 to 1.5
- value_weight: bfloat16 [4096, 1024], P('fsdp', 'tp'), may hold values from -0.09375 to 0.09375
- value_grad: bfloat16 [4096, 1024], P(('rep', 'fsdp'), 'tp'), may hold values from -6 to 6
Outputs:
- input_grad: bfloat16 [4096, 4096], P(('rep', 'fsdp'))
- weight_grad: float32 [4096, 1024], P('fsdp', 'tp')
- gain_grad: float32 [4096], P('fsdp')
The draws below stay inside these ranges and needn't reach their ends.
All inputs are finite; a program needn't handle non-finite values.
Results may differ from the reference program's by a relative error of at most 0.00125.
Values may be sent and summed in bfloat16 or wider, within the bound.
A program may use at most 64 MiB of HBM per device.

```python
import jax
import jax.numpy as jnp
from jax import lax

D = 4096
KV = 1024
TOKENS = 4096
N_REP = 4
N_FSDP = 4


def raised(result, stream_key, source, target, parts, factor):
    def block_of(dim):
        return (jnp.arange(result.shape[dim]) // (result.shape[dim] // parts)).reshape((-1,) + (1,) * (result.ndim - 1 - dim))

    first = jax.random.permutation(stream_key, parts)[block_of(target)]
    other_side = (block_of(target) + parts // 2) % parts
    return jnp.where((block_of(source) == first) | (block_of(source) == other_side), factor * result, result)


def level_of(own_key, extent, pieces, smallest, top_value):
    gain = 1.0
    for position, parts in pieces:
        draws = jax.random.uniform(jax.random.fold_in(jax.random.fold_in(own_key, 6), position), (parts,), jnp.float32, smallest / len(pieces), top_value / len(pieces))
        gain = gain * jnp.repeat(jnp.exp(draws), extent[position] // parts).reshape((-1,) + (1,) * (len(extent) - 1 - position))
    return gain


def centred(stream_key, dims, deviation, reach, shards=(), kind=jnp.bfloat16):
    values = deviation * jax.random.normal(stream_key, dims, jnp.float32)
    if shards:
        values = values * level_of(stream_key, dims, shards, -0.22, 0.18)
    return jnp.clip(values, -reach, reach).astype(kind)


def gaussian_with(stream_key, shape, spread, limit, split, heavy, kind=jnp.bfloat16):
    values = spread * jax.random.normal(stream_key, shape, jnp.float32)
    if split:
        values = values * level_of(stream_key, shape, split, -0.22, 0.18)
    return jnp.clip(raised(values, jax.random.fold_in(stream_key, 3), *heavy), -limit, limit).astype(kind)


def setup_inputs(seed: int = 0) -> dict:
    key_list = jax.random.split(jax.random.key(seed), 5)
    return {
        "hidden": gaussian_with(key_list[0], (TOKENS, D), 1.0, 6.0, ((0, 16),), (0, 1, 16, 2.0)),
        "norm_gain": jnp.clip(1.0 + 0.1 * jax.random.normal(key_list[1], (D,), jnp.float32), 0.5, 1.5),
        "value_weight": centred(key_list[2], (D, KV), D ** -0.5, 0.09375, ((0, 4), (1, 2))),
        "value_grad": centred(key_list[3], (TOKENS, KV), 1.0, 6.0, ((0, 16), (1, 2))),
    }


epsilon = 1e-05

def reference(hidden, norm_gain, value_weight, value_grad):
    inputs = hidden.astype(jnp.float32)
    inv_rms = lax.rsqrt(lax.optimization_barrier(jnp.mean(inputs * inputs, axis=1, keepdims=True)) + epsilon)
    normal = inputs * inv_rms
    normed = (normal * norm_gain).astype(jnp.bfloat16)
    grad_normed = jnp.dot(value_grad, value_weight.T, preferred_element_type=jnp.float32)
    average = 1.0 / (N_REP * N_FSDP)
    weight_grad = jnp.dot(normed.T, value_grad, preferred_element_type=jnp.float32) * average
    gain_grad = lax.optimization_barrier(jnp.sum(grad_normed * normal, axis=0)) * average
    grad_scaled = grad_normed * norm_gain
    center = lax.optimization_barrier(jnp.mean(grad_scaled * normal, axis=1, keepdims=True))
    input_grad = (inv_rms * (grad_scaled - normal * center)).astype(jnp.bfloat16)
    return (input_grad, weight_grad, gain_grad)
```

```python
import functools

import jax
import jax.numpy as jnp
from jax import lax
from jax.experimental import pallas as pl
from jax.experimental.pallas import tpu as pltpu
from jax.sharding import PartitionSpec as P

epsilon = 1e-05
MESH = pl.DeviceIdType.MESH
ROWS = 32
LANES = 128


def kernel(sizes, hid, gain, w, vg, dx, dw, dgain,
           hv, cols, nm, vgs, vgx, wx, invc, inv_rows, gn, rsc, rs, cenc, cg, wp, wr, gacc, gbuf,
           s_load, s_h, r_h, s_hx, r_hx, s_v, r_v, s_vx, r_vx, s_w, r_w, s_i, r_i,
           s_rs, r_rs, s_b, r_b, s_bx, r_bx, s_p, r_p, s_q, r_q, s_g, r_g):
    nrep, n, ntp = sizes
    r, f, c = lax.axis_index("rep"), lax.axis_index("fsdp"), lax.axis_index("tp")
    T, D = hid.shape
    F, K = w.shape
    Th = T // ntp
    Fq = F // nrep
    average = 1.0 / (nrep * n)
    wide = F // LANES

    def remote(src, dst, ssem, rsem, dev):
        return pltpu.make_async_remote_copy(src_ref=src, dst_ref=dst, send_sem=ssem, recv_sem=rsem,
                                            device_id=dev, device_id_type=MESH)

    def half(j, h):
        return pl.ds(pl.multiple_of(j * T + h * Th, LANES), Th)

    def full(j):
        return pl.ds(pl.multiple_of(j * T, LANES), T)

    def feats(j):
        return pl.ds(pl.multiple_of(j * F, LANES), F)

    def tokens(h):
        return pl.ds(pl.multiple_of(h * Th, LANES), Th)

    zpeer = [lax.rem(f + s, n) for s in range(n)]
    tpeer = [lax.rem(c + s, ntp) for s in range(ntp)]
    rpeer = [lax.rem(r + s, nrep) for s in range(nrep)]
    zfrom = [lax.rem(f + n - s, n) for s in range(n)]

    load_h = pltpu.make_async_copy(hid, hv, s_load.at[0])
    load_v = pltpu.make_async_copy(vg, vgs.at[full(f)], s_load.at[1])
    load_w = pltpu.make_async_copy(w, wx.at[c], s_load.at[2])
    load_h.start()
    load_v.start()
    load_w.start()

    barrier = pltpu.get_barrier_semaphore()
    for s in range(1, n):
        pl.semaphore_signal(barrier, inc=1, device_id={"fsdp": zpeer[s]}, device_id_type=MESH)
    for a in range(nrep):
        for b in range(ntp):
            if a or b:
                pl.semaphore_signal(barrier, inc=1, device_id={"rep": rpeer[a], "tp": tpeer[b]}, device_id_type=MESH)
    pl.semaphore_wait(barrier, n - 1 + nrep * ntp - 1)

    def send_v(s):
        return remote(vg, vgs.at[full(f)], s_v.at[s], r_v.at[s], {"fsdp": zpeer[s]})

    def got_v(s):
        return remote(vg, vgs.at[full(zfrom[s])], s_v.at[s], r_v.at[s], {"fsdp": zpeer[s]})

    def send_h(s):
        return remote(hid.at[tokens(c), feats(zpeer[s])], cols.at[half(f, c)], s_h.at[s], r_h.at[s], {"fsdp": zpeer[s]})

    def got_h(s):
        return remote(hid.at[tokens(c), feats(f)], cols.at[half(zfrom[s], c)], s_h.at[s], r_h.at[s], {"fsdp": zpeer[s]})

    def send_i(s):
        return remote(inv_rows.at[f], inv_rows.at[f], s_i.at[s], r_i.at[s], {"fsdp": zpeer[s]})

    def got_i(s):
        return remote(inv_rows.at[f], inv_rows.at[zfrom[s]], s_i.at[s], r_i.at[s], {"fsdp": zpeer[s]})

    def pass_v(s, b):
        j = zfrom[s]
        src = vg.at[tokens(tpeer[b])] if s == 0 else vgs.at[half(j, tpeer[b])]
        return remote(src, vgx.at[b, pl.ds(pl.multiple_of(j * Th, LANES), Th)],
                      s_vx.at[b, s], r_vx.at[b, s], {"tp": tpeer[b]})

    def pass_h(s, b):
        rows = half(zfrom[s], c)
        return remote(cols.at[rows], cols.at[rows], s_hx.at[b, s], r_hx.at[b, s], {"tp": tpeer[b]})

    def took_h(s, b):
        rows = half(zfrom[s], lax.rem(c + ntp - b, ntp))
        return remote(cols.at[rows], cols.at[rows], s_hx.at[b, s], r_hx.at[b, s], {"tp": tpeer[b]})

    def pass_w(b):
        return remote(w, wx.at[c], s_w.at[b], r_w.at[b], {"tp": tpeer[b]})

    def took_w(b):
        return remote(w, wx.at[lax.rem(c + ntp - b, ntp)], s_w.at[b], r_w.at[b], {"tp": tpeer[b]})

    for s in range(1, n):
        send_v(s).start()
    for s in range(1, n):
        send_h(s).start()
    for b in range(1, ntp):
        pass_w(b).start()
        pass_v(0, b).start()

    load_h.wait()

    @pl.loop(0, T // ROWS)
    def _(i):
        rows = pl.ds(pl.multiple_of(i * ROWS, ROWS), ROWS)
        acc = jnp.zeros((ROWS, LANES), jnp.float32)
        for k in range(D // LANES):
            x = hv[rows, k * LANES:(k + 1) * LANES].astype(jnp.float32)
            acc = acc + x * x
        inv = lax.rsqrt(jnp.sum(acc, axis=1, keepdims=True) / D + epsilon)
        invc[pl.ds(pl.multiple_of(f * T + i * ROWS, ROWS), ROWS), :] = jnp.broadcast_to(inv, (ROWS, LANES))

    for k in range(T // LANES):
        block = invc[pl.ds(pl.multiple_of(f * T + k * LANES, LANES), LANES), :]
        inv_rows[f, :, k * LANES:(k + 1) * LANES] = block.T[:8, :]
    for s in range(1, n):
        send_i(s).start()
    cols[full(f), :] = hv[:, feats(f)]

    def spread(x):
        return jnp.concatenate([x] * wide, axis=1) if wide > 1 else x

    gains = gain[...]

    def normalise(first, count):
        @pl.loop(0, count // ROWS)
        def _(i):
            rows = pl.ds(pl.multiple_of(first + i * ROWS, ROWS), ROWS)
            normal = cols[rows, :].astype(jnp.float32) * spread(invc[rows, :])
            nm[rows, :] = (normal * gains).astype(jnp.bfloat16)

    normalise(f * T, T)
    load_v.wait()
    load_w.wait()
    for b in range(1, ntp):
        took_w(b).wait_recv()
        pass_v(0, b).wait_recv()
    gacc[...] = jnp.zeros_like(gacc)

    def products(j):
        vrows = pl.ds(pl.multiple_of(j * Th, LANES), Th)
        total = lax.dot_general(vgs[half(j, c), :], wx[c], (((1,), (1,)), ((), ())), preferred_element_type=jnp.float32)
        for b in range(1, ntp):
            total = total + lax.dot_general(vgx[b, vrows, :], wx[lax.rem(c + ntp - b, ntp)], (((1,), (1,)), ((), ())),
                                            preferred_element_type=jnp.float32)
        gn[vrows, :] = total

        @pl.loop(0, Th // ROWS)
        def _(i):
            rows = pl.ds(pl.multiple_of(j * T + c * Th + i * ROWS, ROWS), ROWS)
            mine = pl.ds(pl.multiple_of(j * Th + i * ROWS, ROWS), ROWS)
            normal = cols[rows, :].astype(jnp.float32) * spread(invc[rows, :])
            t = gn[mine, :] * normal
            gacc[...] += jnp.sum(t.reshape(ROWS // 8, 8, F), axis=0)
            rsc[pl.ds(pl.multiple_of(i * ROWS, ROWS), ROWS), :] = jnp.broadcast_to(
                jnp.sum(t * gains, axis=1, keepdims=True), (ROWS, LANES))

        for k in range(Th // LANES):
            rs[f, pl.ds(j, 1), k * LANES:(k + 1) * LANES] = rsc[k * LANES:(k + 1) * LANES, :].T[:1, :]

    products(f)
    for s in range(1, n):
        got_v(s).wait_recv()
        for b in range(1, ntp):
            pass_v(s, b).start()
    for s in range(1, n):
        j = zfrom[s]
        got_h(s).wait_recv()
        for b in range(1, ntp):
            pass_h(s, b).start()
        got_i(s).wait_recv()
        for k in range(T // LANES):
            row = inv_rows[j, :1, k * LANES:(k + 1) * LANES]
            invc[pl.ds(pl.multiple_of(j * T + k * LANES, LANES), LANES), :] = jnp.broadcast_to(row, (LANES, LANES)).T
        for b in range(1, ntp):
            pass_v(s, b).wait_recv()
            took_h(s, b).wait_recv()
        normalise(j * T, T)

    def quarter(q):
        return pl.ds(pl.multiple_of(q * Fq, 8), Fq)

    def send_p(s):
        return remote(wp.at[quarter(rpeer[s])], wr.at[s], s_p.at[s], r_p.at[s], {"rep": rpeer[s]})

    def partial_of(columns):
        return lax.dot_general(nm[:, columns], vgs[...], (((0,), (0,)), ((), ())), preferred_element_type=jnp.float32)

    if Fq % LANES == 0:
        for s in [*range(1, nrep), 0]:
            q = rpeer[s]
            wp[quarter(q), :] = partial_of(pl.ds(pl.multiple_of(q * Fq, LANES), Fq))
            if s:
                send_p(s).start()
    else:
        wp[...] = partial_of(slice(None))
        for s in range(1, nrep):
            send_p(s).start()

    for s in range(1, n):
        products(zfrom[s])

    def send_rs(s):
        return remote(rs.at[f], rs.at[f], s_rs.at[s], r_rs.at[s], {"fsdp": zpeer[s]})

    def got_rs(s):
        return remote(rs.at[f], rs.at[zfrom[s]], s_rs.at[s], r_rs.at[s], {"fsdp": zpeer[s]})

    for s in range(1, n):
        send_rs(s).start()

    slot = r * ntp + c
    gbuf[slot] = jnp.sum(gacc[...], axis=0, keepdims=True)

    def send_g(a, b):
        return remote(gbuf.at[slot], gbuf.at[slot], s_g.at[a, b], r_g.at[a, b], {"rep": rpeer[a], "tp": tpeer[b]})

    def got_g(a, b):
        src = lax.rem(r + nrep - a, nrep) * ntp + lax.rem(c + ntp - b, ntp)
        return remote(gbuf.at[slot], gbuf.at[src], s_g.at[a, b], r_g.at[a, b], {"rep": rpeer[a], "tp": tpeer[b]})

    others = [(a, b) for a in range(nrep) for b in range(ntp) if a or b]
    for a, b in others:
        send_g(a, b).start()

    for s in range(1, n):
        got_rs(s).wait_recv()
    center = rs[0]
    for s in range(1, n):
        center = center + rs[s]
    rs_total = center / D
    rsc_rows = rs_total.shape[0]

    def send_b(s):
        return remote(cg.at[pl.ds(pl.multiple_of(zpeer[s] * Th, LANES), Th)], dx.at[tokens(c), feats(f)],
                      s_b.at[s], r_b.at[s], {"fsdp": zpeer[s]})

    def got_b(s):
        return remote(cg.at[pl.ds(0, Th)], dx.at[tokens(c), feats(zfrom[s])],
                      s_b.at[s], r_b.at[s], {"fsdp": zpeer[s]})

    def pass_b(s, b):
        ref = dx.at[tokens(c), feats(zfrom[s])]
        return remote(ref, ref, s_bx.at[b, s], r_bx.at[b, s], {"tp": tpeer[b]})

    def took_b(s, b):
        ref = dx.at[tokens(lax.rem(c + ntp - b, ntp)), feats(zfrom[s])]
        return remote(ref, ref, s_bx.at[b, s], r_bx.at[b, s], {"tp": tpeer[b]})

    cenc[...] = rs_total
    for s in [*range(1, n), 0]:
        j = zpeer[s]
        for k in range(Th // LANES):
            row = cenc[pl.ds(j, 1), k * LANES:(k + 1) * LANES]
            rsc[k * LANES:(k + 1) * LANES, :] = jnp.broadcast_to(row, (LANES, LANES)).T

        @pl.loop(0, Th // ROWS)
        def _(i):
            rows = pl.ds(pl.multiple_of(j * T + c * Th + i * ROWS, ROWS), ROWS)
            mine = pl.ds(pl.multiple_of(j * Th + i * ROWS, ROWS), ROWS)
            inv = spread(invc[rows, :])
            normal = cols[rows, :].astype(jnp.float32) * inv
            cen = spread(rsc[pl.ds(pl.multiple_of(i * ROWS, ROWS), ROWS), :])
            cg[mine, :] = (inv * (gn[mine, :] * gains - normal * cen)).astype(jnp.bfloat16)

        if s:
            send_b(s).start()
        else:
            dx[tokens(c), feats(f)] = cg[pl.ds(pl.multiple_of(f * Th, LANES), Th), :]
            for b in range(1, ntp):
                pass_b(0, b).start()

    def send_q(s):
        return remote(dw.at[quarter(r)], dw.at[quarter(r)], s_q.at[s], r_q.at[s], {"rep": rpeer[s]})

    def got_q(s):
        ref = dw.at[quarter(lax.rem(r + nrep - s, nrep))]
        return remote(ref, ref, s_q.at[s], r_q.at[s], {"rep": rpeer[s]})

    for s in range(1, nrep):
        send_p(s).wait_recv()
    total = wp[quarter(r), :]
    for s in range(1, nrep):
        total = total + wr[s]
    dw[quarter(r), :] = total * average
    for s in range(1, nrep):
        send_q(s).start()

    for a, b in others:
        got_g(a, b).wait_recv()
    gsum = gbuf[0]
    for i in range(1, nrep * ntp):
        gsum = gsum + gbuf[i]
    dgain[...] = gsum * average

    for s in range(1, n):
        got_b(s).wait_recv()
        for b in range(1, ntp):
            pass_b(s, b).start()
    for s in range(1, nrep):
        got_q(s).wait_recv()
    for s in range(n):
        for b in range(1, ntp):
            took_b(s, b).wait_recv()
    for s in range(1, n):
        for copy in (send_v(s), send_h(s), send_i(s), send_rs(s), send_b(s)):
            copy.wait_send()
    for s in range(1, nrep):
        send_p(s).wait_send()
        send_q(s).wait_send()
    for a, b in others:
        send_g(a, b).wait_send()
    for b in range(1, ntp):
        pass_w(b).wait_send()
        for s in range(n):
            pass_v(s, b).wait_send()
            pass_b(s, b).wait_send()
            if s:
                pass_h(s, b).wait_send()


def shards(hidden, norm_gain, value_weight, value_grad):
    nrep, n, ntp = (lax.axis_size(a) for a in ("rep", "fsdp", "tp"))
    T, D = hidden.shape
    F, K = value_weight.shape
    Th, Fq = T // ntp, F // nrep
    G = n * T
    n8 = -(-n // 8) * 8
    dma = pltpu.SemaphoreType.DMA
    f32, bf16 = jnp.float32, jnp.bfloat16
    V = pltpu.VMEM
    vmem = pl.BlockSpec(memory_space=pltpu.VMEM)
    hbm = pl.BlockSpec(memory_space=pl.ANY)
    dx, dw, dgain = pl.pallas_call(
        functools.partial(kernel, (nrep, n, ntp)),
        out_shape=(jax.ShapeDtypeStruct((T, D), bf16), jax.ShapeDtypeStruct((F, K), f32),
                   jax.ShapeDtypeStruct((1, F), f32)),
        in_specs=[hbm, vmem, hbm, hbm],
        out_specs=(vmem, vmem, vmem),
        scratch_shapes=[
            V((T, D), bf16), V((G, F), bf16), V((G, F), bf16), V((G, K), bf16), V((ntp, n * Th, K), bf16),
            V((ntp, F, K), bf16), V((G, LANES), f32), V((n, 8, T), f32), V((n * Th, F), f32), V((Th, LANES), f32),
            V((n, n8, Th), f32), V((n8, Th), f32), V((n * Th, F), bf16), V((F, K), f32), V((nrep, Fq, K), f32),
            V((8, F), f32), V((nrep * ntp, 1, F), f32),
            dma((3,)), dma((n,)), dma((n,)), dma((ntp, n)), dma((ntp, n)), dma((n,)), dma((n,)),
            dma((ntp, n)), dma((ntp, n)), dma((ntp,)), dma((ntp,)), dma((n,)), dma((n,)),
            dma((n,)), dma((n,)), dma((n,)), dma((n,)), dma((ntp, n)), dma((ntp, n)),
            dma((nrep,)), dma((nrep,)), dma((nrep,)), dma((nrep,)), dma((nrep, ntp)), dma((nrep, ntp)),
        ],
        compiler_params=pltpu.CompilerParams(collective_id=0, has_side_effects=True, vmem_limit_bytes=60 * 1024 * 1024),
    )(hidden, norm_gain.reshape(1, F), value_weight, value_grad)
    return dx, dw, dgain.reshape(F)


def solution(mesh):
    placed = (P(("rep", "fsdp"), None), P("fsdp"), P("fsdp", "tp"), P(("rep", "fsdp"), "tp"))
    return jax.shard_map(
        shards,
        mesh=mesh,
        in_specs=placed,
        out_specs=(P(("rep", "fsdp"), None), P("fsdp", "tp"), P("fsdp")),
        check_vma=False,
    )
```

```python
import functools

import jax
import jax.numpy as jnp
from jax import lax
from jax.experimental import pallas as pl
from jax.experimental.pallas import tpu as pltpu
from jax.sharding import PartitionSpec as P

epsilon = 1e-05
MESH = pl.DeviceIdType.MESH
ROWS = 32
LANES = 128


def factor(count):
    small = 1
    for d in range(1, count + 1):
        if count % d == 0 and d * d <= count:
            small = d
    return count // small, small


def chunks_of(F):
    for count in (4, 2):
        if F % (count * LANES) == 0:
            return count
    return 1


def kernel(sizes, hid, gain, w, vg, dx, dw, dgain,
           hv, cols, nm, vgs, vgx, wx, invc, inv_rows, gn, rsc, rs, cenc, cg, wp, wr1, ws1, wr2, gacc, gbuf,
           s_load, s_h, r_h, s_hx, r_hx, s_v, r_v, s_vx, r_vx, s_w, r_w, s_i, r_i,
           s_rs, r_rs, s_b, r_b, s_bx, r_bx, s_p, r_p, s_g, r_g):
    nrep, n, ntp = sizes
    r, f, c = lax.axis_index("rep"), lax.axis_index("fsdp"), lax.axis_index("tp")
    T, D = hid.shape
    F, K = w.shape
    Th = T // ntp
    C = chunks_of(F)
    Fc = F // C
    average = 1.0 / (nrep * n)
    wide = Fc // LANES
    nt = (((1,), (1,)), ((), ()))
    tn = (((0,), (0,)), ((), ()))

    def remote(src, dst, ssem, rsem, dev):
        return pltpu.make_async_remote_copy(src_ref=src, dst_ref=dst, send_sem=ssem, recv_sem=rsem,
                                            device_id=dev, device_id_type=MESH)

    def span(start, count, unit=LANES):
        return pl.ds(pl.multiple_of(start, unit), count)

    def half(j, h):
        return span(j * T + h * Th, Th)

    def full(j):
        return span(j * T, T)

    def tokens(h):
        return span(h * Th, Th)

    def mine(j):
        return span(j * Th, Th)

    def chunk(q):
        return slice(q * Fc, (q + 1) * Fc)

    zpeer = [lax.rem(f + s, n) for s in range(n)]
    zfrom = [lax.rem(f + n - s, n) for s in range(n)]
    tpeer = [lax.rem(c + s, ntp) for s in range(ntp)]
    tfrom = [lax.rem(c + ntp - s, ntp) for s in range(ntp)]
    rpeer = [lax.rem(r + s, nrep) for s in range(nrep)]

    load_h = pltpu.make_async_copy(hid, hv, s_load.at[0])
    load_v = pltpu.make_async_copy(vg, vgs.at[full(f)], s_load.at[1])
    load_w = pltpu.make_async_copy(w, wx.at[c], s_load.at[2])
    load_h.start()
    load_v.start()
    load_w.start()

    barrier = pltpu.get_barrier_semaphore()
    for s in range(1, n):
        pl.semaphore_signal(barrier, inc=1, device_id={"fsdp": zpeer[s]}, device_id_type=MESH)
    for a in range(nrep):
        for b in range(ntp):
            if a or b:
                pl.semaphore_signal(barrier, inc=1, device_id={"rep": rpeer[a], "tp": tpeer[b]}, device_id_type=MESH)
    pl.semaphore_wait(barrier, n - 1 + nrep * ntp - 1)

    def hop_v(d, right):
        j = f - d if right else f + d
        src = vg if d == 0 else vgs.at[full(j)]
        return remote(src, vgs.at[full(j)], s_v.at[int(right), d], r_v.at[j], {"fsdp": f + 1 if right else f - 1})

    def has_v(d, right):
        return f - d >= 0 if right else f + d < n

    def sends_v(d, right):
        return jnp.logical_and(has_v(d, right), f + 1 < n if right else f >= 1)

    def pass_v(j, b, own=False):
        src = vg.at[tokens(tpeer[b])] if own else vgs.at[half(j, tpeer[b])]
        return remote(src, vgx.at[b, mine(j)], s_vx.at[b, j], r_vx.at[b, j], {"tp": tpeer[b]})

    def send_h(q, s):
        columns = span(zpeer[s] * F + q * Fc, Fc)
        return remote(hid.at[tokens(c), columns], cols.at[half(f, c), chunk(q)], s_h.at[q, s], r_h.at[q, s], {"fsdp": zpeer[s]})

    def got_h(q, s):
        ref = cols.at[half(zfrom[s], c), chunk(q)]
        return remote(ref, ref, s_h.at[q, s], r_h.at[q, s], {"fsdp": zpeer[s]})

    def pass_h(q, s, b):
        ref = cols.at[half(zfrom[s], c), chunk(q)]
        return remote(ref, ref, s_hx.at[b, q * n + s], r_hx.at[b, q * n + s], {"tp": tpeer[b]})

    def took_h(q, s, b):
        ref = cols.at[half(zfrom[s], tfrom[b]), chunk(q)]
        return remote(ref, ref, s_hx.at[b, q * n + s], r_hx.at[b, q * n + s], {"tp": tpeer[b]})

    def send_i(s):
        return remote(inv_rows.at[f], inv_rows.at[f], s_i.at[s], r_i.at[s], {"fsdp": zpeer[s]})

    def got_i(s):
        ref = inv_rows.at[zfrom[s]]
        return remote(ref, ref, s_i.at[s], r_i.at[s], {"fsdp": zpeer[s]})

    def pass_w(b):
        return remote(w, wx.at[c], s_w.at[b], r_w.at[b], {"tp": tpeer[b]})

    def took_w(b):
        ref = wx.at[tfrom[b]]
        return remote(ref, ref, s_w.at[b], r_w.at[b], {"tp": tpeer[b]})

    def arrive_v(d):
        for right in (True, False):
            @pl.when(has_v(d, right))
            def _():
                j = f - d if right else f + d
                hop_v(d, right).wait_recv()
                for b in range(1, ntp):
                    pass_v(j, b).start()

            @pl.when(sends_v(d, right))
            def _():
                hop_v(d, right).start()

    for right in (True, False):
        @pl.when(sends_v(0, right))
        def _():
            hop_v(0, right).start()
    for b in range(1, ntp):
        pass_w(b).start()
        pass_v(f, b, True).start()

    load_h.wait()

    @pl.loop(0, T // ROWS)
    def _(i):
        rows = span(i * ROWS, ROWS, ROWS)
        acc = jnp.zeros((ROWS, LANES), jnp.float32)
        for k in range(D // LANES):
            x = hv[rows, k * LANES:(k + 1) * LANES].astype(jnp.float32)
            acc = acc + x * x
        inv = lax.rsqrt(jnp.sum(acc, axis=1, keepdims=True) / D + epsilon)
        invc[span(f * T + i * ROWS, ROWS, ROWS), :] = jnp.broadcast_to(inv, (ROWS, LANES))

    for k in range(T // LANES):
        inv_rows[f, :, k * LANES:(k + 1) * LANES] = invc[span(f * T + k * LANES, LANES), :].T[:8, :]
    for s in range(1, n):
        send_i(s).start()
    order = sorted(range(1, n), key=lambda s: -abs(2 * s - n))
    if n > 1:
        arrive_v(1)
    for s in order:
        send_h(0, s).start()
    for d in range(2, n):
        arrive_v(d)
    for q in range(1, C):
        for s in order:
            send_h(q, s).start()

    cols[full(f), :] = hv[:, span(f * F, F)]
    load_v.wait()
    load_w.wait()
    for j in range(n):
        vgx[0, mine(j), :] = vgs[half(j, c), :]
    for s in range(1, n):
        j = zfrom[s]
        got_i(s).wait_recv()
        for k in range(T // LANES):
            row = inv_rows[j, :1, k * LANES:(k + 1) * LANES]
            invc[span(j * T + k * LANES, LANES), :] = jnp.broadcast_to(row, (LANES, LANES)).T
    gacc[...] = jnp.zeros_like(gacc)
    rsc[...] = jnp.zeros_like(rsc)

    def spread(x, count=wide):
        return jnp.concatenate([x] * count, axis=1) if count > 1 else x

    def arrive_h(q):
        for s in order:
            got_h(q, s).wait_recv()
            for b in range(1, ntp):
                pass_h(q, s, b).start()

    def products(q):
        gains = gain[:, chunk(q)]
        for b in range(ntp):
            part = lax.dot_general(vgx[b], wx[tfrom[b], chunk(q), :], nt, preferred_element_type=jnp.float32)
            gn[:, chunk(q)] = part if b == 0 else gn[:, chunk(q)] + part

        @pl.loop(0, n)
        def _(j):
            @pl.loop(0, Th // ROWS)
            def _(i):
                rows = span(j * T + c * Th + i * ROWS, ROWS, ROWS)
                here = span(j * Th + i * ROWS, ROWS, ROWS)
                t = gn[here, chunk(q)] * (cols[rows, chunk(q)].astype(jnp.float32) * spread(invc[rows, :]))
                gacc[:, chunk(q)] += jnp.sum(t.reshape(ROWS // 8, 8, Fc), axis=0)
                scaled = t * gains
                part = scaled[:, :LANES]
                for k in range(1, wide):
                    part = part + scaled[:, k * LANES:(k + 1) * LANES]
                rsc[here, :] += part

    def partial(q):
        gains = gain[:, chunk(q)]

        @pl.loop(0, n * T // ROWS)
        def _(i):
            rows = span(i * ROWS, ROWS, ROWS)
            normal = cols[rows, chunk(q)].astype(jnp.float32) * spread(invc[rows, :])
            nm[rows, chunk(q)] = (normal * gains).astype(jnp.bfloat16)

        wp[chunk(q), :] = lax.dot_general(nm[:, chunk(q)], vgs[...], tn, preferred_element_type=jnp.float32)

    A, B = factor(nrep)
    ra, rb = r // B, lax.rem(r, B)
    Fh = Fc // 2

    def axes(o):
        first = (rb, B, lambda i: {"rep": ra * B + i})
        second = (ra, A, lambda i: {"rep": i * B + rb})
        return (first, second) if o == 0 else (second, first)

    def rows1(q, o, i):
        size = Fh // axes(o)[0][1]
        return span(q * Fc + o * Fh + i * size, size, 8)

    def rows2(q, o, i):
        size = Fh // nrep
        return span(q * Fc + o * Fh + axes(o)[0][0] * (size * axes(o)[1][1]) + i * size, size, 8)

    def copy_p(stage, q, o, s):
        first, second = axes(o)
        mine_at, count, dev = (first, second, second, first)[stage]
        to = lax.rem(mine_at + s, count)
        if stage == 0:
            src, dst = wp.at[rows1(q, o, to)], wr1.at[q, o, s, :Fh // first[1]]
        elif stage == 1:
            size = Fh // nrep
            src, dst = ws1.at[q, o, span(to * size, size, 8)], wr2.at[q, o, s]
        elif stage == 2:
            src = dst = dw.at[rows2(q, o, mine_at)]
        else:
            src = dst = dw.at[rows1(q, o, mine_at)]
        at = (stage * C + q) * 2 + o
        return remote(src, dst, s_p.at[at, s], r_p.at[at, s], dev(to))

    def got_p(stage, q, o, s):
        first, second = axes(o)
        mine_at, count, dev = (first, second, second, first)[stage]
        source = lax.rem(mine_at + count - s, count)
        at = (stage * C + q) * 2 + o
        if stage == 0:
            ref = wr1.at[q, o, s, :Fh // first[1]]
        elif stage == 1:
            ref = wr2.at[q, o, s]
        elif stage == 2:
            ref = dw.at[rows2(q, o, source)]
        else:
            ref = dw.at[rows1(q, o, source)]
        return remote(ref, ref, s_p.at[at, s], r_p.at[at, s], dev(lax.rem(mine_at + s, count)))

    def counts(stage, o):
        first, second = axes(o)
        return (first, second, second, first)[stage][1]

    def stage_p(stage, q):
        for o in range(2):
            first, second = axes(o)
            if stage:
                for s in range(1, counts(stage - 1, o)):
                    got_p(stage - 1, q, o, s).wait_recv()
            if stage == 1:
                total = wp[rows1(q, o, first[0]), :]
                for s in range(1, first[1]):
                    total = total + wr1[q, o, s, :Fh // first[1]]
                ws1[q, o, :Fh // first[1]] = total
            elif stage == 2:
                size = Fh // nrep
                total = ws1[q, o, span(second[0] * size, size, 8)]
                for s in range(1, second[1]):
                    total = total + wr2[q, o, s]
                dw[rows2(q, o, second[0]), :] = total * average
            if stage < 4:
                for s in range(1, counts(stage, o)):
                    copy_p(stage, q, o, s).start()

    done = [0] * C

    def advance(steps):
        for q, upto in steps:
            while done[q] < upto:
                stage_p(done[q], q)
                done[q] += 1

    def send_rs(s):
        return remote(rs.at[f], rs.at[f], s_rs.at[s], r_rs.at[s], {"fsdp": zpeer[s]})

    def got_rs(s):
        ref = rs.at[zfrom[s]]
        return remote(ref, ref, s_rs.at[s], r_rs.at[s], {"fsdp": zpeer[s]})

    for b in range(1, ntp):
        took_w(b).wait_recv()
        for j in range(n):
            pass_v(j, b).wait_recv()

    for q in range(C):
        arrive_h(q)
        if q == C - 1:
            products(q)
            for j in range(n):
                for k in range(Th // LANES):
                    block = rsc[span(j * Th + k * LANES, LANES), :].T
                    rs[f, j:j + 1, k * LANES:(k + 1) * LANES] = jnp.sum(block, axis=0, keepdims=True)
            for s in range(1, n):
                send_rs(s).start()
        for s in order:
            for b in range(1, ntp):
                took_h(q, s, b).wait_recv()
        partial(q)
        advance([(q, 1)])
        if q < C - 1:
            products(q)
        advance([(p, q - p + 1) for p in range(q)])

    slot = r * ntp + c
    gbuf[slot] = jnp.sum(gacc[...], axis=0, keepdims=True)

    def send_g(a, b):
        return remote(gbuf.at[slot], gbuf.at[slot], s_g.at[a, b], r_g.at[a, b], {"rep": rpeer[a], "tp": tpeer[b]})

    def got_g(a, b):
        ref = gbuf.at[lax.rem(r + nrep - a, nrep) * ntp + tfrom[b]]
        return remote(ref, ref, s_g.at[a, b], r_g.at[a, b], {"rep": rpeer[a], "tp": tpeer[b]})

    others = [(a, b) for a in range(nrep) for b in range(ntp) if a or b]
    for a, b in others:
        send_g(a, b).start()

    for s in range(1, n):
        got_rs(s).wait_recv()
    center = rs[0, :n, :]
    for s in range(1, n):
        center = center + rs[s, :n, :]
    cenc[:n, :] = center / D

    def send_b(s):
        return remote(cg.at[mine(zpeer[s])], dx.at[tokens(c), span(f * F, F)], s_b.at[s], r_b.at[s], {"fsdp": zpeer[s]})

    def got_b(s):
        ref = dx.at[tokens(c), span(zfrom[s] * F, F)]
        return remote(ref, ref, s_b.at[s], r_b.at[s], {"fsdp": zpeer[s]})

    def pass_b(s, b):
        ref = dx.at[tokens(c), span(zfrom[s] * F, F)]
        return remote(ref, ref, s_bx.at[b, s], r_bx.at[b, s], {"tp": tpeer[b]})

    def took_b(s, b):
        ref = dx.at[tokens(tfrom[b]), span(zfrom[s] * F, F)]
        return remote(ref, ref, s_bx.at[b, s], r_bx.at[b, s], {"tp": tpeer[b]})

    for s in [*order, 0]:
        j = zpeer[s]
        for k in range(Th // LANES):
            row = cenc[pl.ds(j, 1), k * LANES:(k + 1) * LANES]
            rsc[k * LANES:(k + 1) * LANES, :] = jnp.broadcast_to(row, (LANES, LANES)).T

        @pl.loop(0, Th // ROWS)
        def _(i):
            rows = span(j * T + c * Th + i * ROWS, ROWS, ROWS)
            here = span(j * Th + i * ROWS, ROWS, ROWS)
            inv, cen = invc[rows, :], rsc[span(i * ROWS, ROWS, ROWS), :]
            for q in range(C):
                scale = spread(inv)
                normal = cols[rows, chunk(q)].astype(jnp.float32) * scale
                cg[here, chunk(q)] = (scale * (gn[here, chunk(q)] * gain[:, chunk(q)] - normal * spread(cen))).astype(jnp.bfloat16)

        if s:
            send_b(s).start()
        else:
            dx[tokens(c), span(f * F, F)] = cg[mine(f), :]
            for b in range(1, ntp):
                pass_b(0, b).start()

    for stage in range(2, 5):
        advance([(q, min(5, max(done[q] + 1, stage))) for q in range(C)])
    for a, b in others:
        got_g(a, b).wait_recv()
    gsum = gbuf[0]
    for i in range(1, nrep * ntp):
        gsum = gsum + gbuf[i]
    dgain[...] = gsum * average

    for s in order:
        got_b(s).wait_recv()
        for b in range(1, ntp):
            pass_b(s, b).start()
    advance([(q, 5) for q in range(C)])
    for s in range(n):
        for b in range(1, ntp):
            took_b(s, b).wait_recv()
    for d in range(n):
        for right in (True, False):
            @pl.when(sends_v(d, right))
            def _():
                hop_v(d, right).wait_send()
    for s in range(1, n):
        for copy in (send_i(s), send_rs(s), send_b(s), *[send_h(q, s) for q in range(C)]):
            copy.wait_send()
    for q in range(C):
        for o in range(2):
            for stage in range(4):
                for s in range(1, counts(stage, o)):
                    copy_p(stage, q, o, s).wait_send()
    for a, b in others:
        send_g(a, b).wait_send()
    for b in range(1, ntp):
        pass_w(b).wait_send()
        for s in range(n):
            pass_v(s, b).wait_send()
            pass_b(s, b).wait_send()
            if s:
                for q in range(C):
                    pass_h(q, s, b).wait_send()


def shards(hidden, norm_gain, value_weight, value_grad):
    nrep, n, ntp = (lax.axis_size(a) for a in ("rep", "fsdp", "tp"))
    T, D = hidden.shape
    F, K = value_weight.shape
    Th = T // ntp
    C = chunks_of(F)
    Fh = F // C // 2
    A, B = factor(nrep)
    G = n * T
    n8 = -(-n // 8) * 8
    dma = pltpu.SemaphoreType.DMA
    f32, bf16 = jnp.float32, jnp.bfloat16
    V = pltpu.VMEM
    vmem = pl.BlockSpec(memory_space=pltpu.VMEM)
    hbm = pl.BlockSpec(memory_space=pl.ANY)
    dx, dw, dgain = pl.pallas_call(
        functools.partial(kernel, (nrep, n, ntp)),
        out_shape=(jax.ShapeDtypeStruct((T, D), bf16), jax.ShapeDtypeStruct((F, K), f32),
                   jax.ShapeDtypeStruct((1, F), f32)),
        in_specs=[hbm, vmem, hbm, hbm],
        out_specs=(vmem, vmem, vmem),
        scratch_shapes=[
            V((T, D), bf16), V((G, F), bf16), V((G, F), bf16), V((G, K), bf16), V((ntp, n * Th, K), bf16),
            V((ntp, F, K), bf16), V((G, LANES), f32), V((n, 8, T), f32), V((n * Th, F), f32), V((n * Th, LANES), f32),
            V((n, n8, Th), f32), V((n8, Th), f32), V((n * Th, F), bf16), V((F, K), f32),
            V((C, 2, A, Fh // B, K), f32), V((C, 2, Fh // B, K), f32), V((C, 2, A, Fh // nrep, K), f32),
            V((8, F), f32), V((nrep * ntp, 1, F), f32),
            dma((3,)), dma((C, n)), dma((C, n)), dma((ntp, C * n)), dma((ntp, C * n)), dma((2, n)), dma((n,)),
            dma((ntp, n)), dma((ntp, n)), dma((ntp,)), dma((ntp,)), dma((n,)), dma((n,)),
            dma((n,)), dma((n,)), dma((n,)), dma((n,)), dma((ntp, n)), dma((ntp, n)),
            dma((8 * C, A)), dma((8 * C, A)), dma((nrep, ntp)), dma((nrep, ntp)),
        ],
        compiler_params=pltpu.CompilerParams(collective_id=0, has_side_effects=True, vmem_limit_bytes=60 * 1024 * 1024),
    )(hidden, norm_gain.reshape(1, F), value_weight, value_grad)
    return dx, dw, dgain.reshape(F)


def solution(mesh):
    placed = (P(("rep", "fsdp"), None), P("fsdp"), P("fsdp", "tp"), P(("rep", "fsdp"), "tp"))
    return jax.shard_map(
        shards,
        mesh=mesh,
        in_specs=placed,
        out_specs=(P(("rep", "fsdp"), None), P("fsdp", "tp"), P("fsdp")),
        check_vma=False,
    )
```

```python
import functools

import jax
import jax.numpy as jnp
from jax import lax
from jax.experimental import pallas as pl
from jax.experimental.pallas import tpu as pltpu
from jax.sharding import PartitionSpec as P

epsilon = 1e-05
MESH = pl.DeviceIdType.MESH
ROWS = 32
LANES = 128


def factor(count):
    small = 1
    for d in range(1, count + 1):
        if count % d == 0 and d * d <= count:
            small = d
    return count // small, small


def chunks_of(F):
    for count in (4, 2):
        if F % (count * LANES) == 0:
            return count
    return 1


def kernel(sizes, hid, gain, w, vg, dx, dw, dgain,
           hv, cols, nm, vgs, vgx, wx, invc, inv_rows, gn, rsc, rs, cenc, cg, wp, wr1, ws1, wr2, gacc, gbuf,
           s_load, s_h, r_h, s_hx, r_hx, s_v, r_v, s_vx, r_vx, s_w, r_w, s_i, r_i,
           s_rs, r_rs, s_b, r_b, s_bx, r_bx, s_p, r_p, s_g, r_g):
    nrep, n, ntp = sizes
    r, f, c = lax.axis_index("rep"), lax.axis_index("fsdp"), lax.axis_index("tp")
    T, D = hid.shape
    F, K = w.shape
    Th = T // ntp
    C = chunks_of(F)
    Fc = F // C
    average = 1.0 / (nrep * n)
    wide = Fc // LANES
    nt = (((1,), (1,)), ((), ()))
    tn = (((0,), (0,)), ((), ()))

    def remote(src, dst, ssem, rsem, dev):
        return pltpu.make_async_remote_copy(src_ref=src, dst_ref=dst, send_sem=ssem, recv_sem=rsem,
                                            device_id=dev, device_id_type=MESH)

    def span(start, count, unit=LANES):
        return pl.ds(pl.multiple_of(start, unit), count)

    def half(j, h):
        return span(j * T + h * Th, Th)

    def full(j):
        return span(j * T, T)

    def tokens(h):
        return span(h * Th, Th)

    def mine(j):
        return span(j * Th, Th)

    def chunk(q):
        return slice(q * Fc, (q + 1) * Fc)

    zpeer = [lax.rem(f + s, n) for s in range(n)]
    zfrom = [lax.rem(f + n - s, n) for s in range(n)]
    tpeer = [lax.rem(c + s, ntp) for s in range(ntp)]
    tfrom = [lax.rem(c + ntp - s, ntp) for s in range(ntp)]
    rpeer = [lax.rem(r + s, nrep) for s in range(nrep)]

    load_h = pltpu.make_async_copy(hid, hv, s_load.at[0])
    load_v = pltpu.make_async_copy(vg, vgs.at[full(f)], s_load.at[1])
    load_w = pltpu.make_async_copy(w, wx.at[c], s_load.at[2])
    load_h.start()
    load_v.start()
    load_w.start()

    barrier = pltpu.get_barrier_semaphore()
    for s in range(1, n):
        pl.semaphore_signal(barrier, inc=1, device_id={"fsdp": zpeer[s]}, device_id_type=MESH)
    for a in range(nrep):
        for b in range(ntp):
            if a or b:
                pl.semaphore_signal(barrier, inc=1, device_id={"rep": rpeer[a], "tp": tpeer[b]}, device_id_type=MESH)
    pl.semaphore_wait(barrier, n - 1 + nrep * ntp - 1)

    def hop_v(d, right):
        j = f - d if right else f + d
        src = vg if d == 0 else vgs.at[full(j)]
        return remote(src, vgs.at[full(j)], s_v.at[int(right), d], r_v.at[j], {"fsdp": f + 1 if right else f - 1})

    def has_v(d, right):
        return f - d >= 0 if right else f + d < n

    def sends_v(d, right):
        return jnp.logical_and(has_v(d, right), f + 1 < n if right else f >= 1)

    def pass_v(j, b, own=False):
        src = vg.at[tokens(tpeer[b])] if own else vgs.at[half(j, tpeer[b])]
        return remote(src, vgx.at[b, mine(j)], s_vx.at[b, j], r_vx.at[b, j], {"tp": tpeer[b]})

    def send_h(q, s):
        columns = span(zpeer[s] * F + q * Fc, Fc)
        return remote(hid.at[tokens(c), columns], cols.at[half(f, c), chunk(q)], s_h.at[q, s], r_h.at[q, s], {"fsdp": zpeer[s]})

    def got_h(q, s):
        ref = cols.at[half(zfrom[s], c), chunk(q)]
        return remote(ref, ref, s_h.at[q, s], r_h.at[q, s], {"fsdp": zpeer[s]})

    def pass_h(q, s, b):
        ref = cols.at[half(zfrom[s], c), chunk(q)]
        return remote(ref, ref, s_hx.at[b, q * n + s], r_hx.at[b, q * n + s], {"tp": tpeer[b]})

    def took_h(q, s, b):
        ref = cols.at[half(zfrom[s], tfrom[b]), chunk(q)]
        return remote(ref, ref, s_hx.at[b, q * n + s], r_hx.at[b, q * n + s], {"tp": tpeer[b]})

    def send_i(s):
        return remote(inv_rows.at[f], inv_rows.at[f], s_i.at[s], r_i.at[s], {"fsdp": zpeer[s]})

    def got_i(s):
        ref = inv_rows.at[zfrom[s]]
        return remote(ref, ref, s_i.at[s], r_i.at[s], {"fsdp": zpeer[s]})

    def pass_w(b):
        return remote(w, wx.at[c], s_w.at[b], r_w.at[b], {"tp": tpeer[b]})

    def took_w(b):
        ref = wx.at[tfrom[b]]
        return remote(ref, ref, s_w.at[b], r_w.at[b], {"tp": tpeer[b]})

    def arrive_v(d):
        for right in (True, False):
            @pl.when(has_v(d, right))
            def _():
                j = f - d if right else f + d
                hop_v(d, right).wait_recv()
                for b in range(1, ntp):
                    pass_v(j, b).start()

            @pl.when(sends_v(d, right))
            def _():
                hop_v(d, right).start()

    for right in (True, False):
        @pl.when(sends_v(0, right))
        def _():
            hop_v(0, right).start()
    order = list(range(1, n))
    for s in order:
        send_h(0, s).start()
    for b in range(1, ntp):
        pass_w(b).start()
        pass_v(f, b, True).start()

    load_h.wait()

    @pl.loop(0, T // ROWS)
    def _(i):
        rows = span(i * ROWS, ROWS, ROWS)
        acc = jnp.zeros((ROWS, LANES), jnp.float32)
        for k in range(D // LANES):
            x = hv[rows, k * LANES:(k + 1) * LANES].astype(jnp.float32)
            acc = acc + x * x
        inv = lax.rsqrt(jnp.sum(acc, axis=1, keepdims=True) / D + epsilon)
        invc[span(f * T + i * ROWS, ROWS, ROWS), :] = jnp.broadcast_to(inv, (ROWS, LANES))

    for k in range(T // LANES):
        inv_rows[f, :, k * LANES:(k + 1) * LANES] = invc[span(f * T + k * LANES, LANES), :].T[:8, :]
    for s in range(1, n):
        send_i(s).start()
    for d in range(1, max(n, C)):
        if d < n:
            arrive_v(d)
        if d < C:
            for s in order:
                send_h(d, s).start()

    cols[full(f), :] = hv[:, span(f * F, F)]
    load_v.wait()
    load_w.wait()
    for j in range(n):
        vgx[0, mine(j), :] = vgs[half(j, c), :]
    for s in range(1, n):
        j = zfrom[s]
        got_i(s).wait_recv()
        for k in range(T // LANES):
            row = inv_rows[j, :1, k * LANES:(k + 1) * LANES]
            invc[span(j * T + k * LANES, LANES), :] = jnp.broadcast_to(row, (LANES, LANES)).T
    gacc[...] = jnp.zeros_like(gacc)
    rsc[...] = jnp.zeros_like(rsc)

    def spread(x, count=wide):
        return jnp.concatenate([x] * count, axis=1) if count > 1 else x

    def arrive_h(q):
        for s in order:
            got_h(q, s).wait_recv()
            for b in range(1, ntp):
                pass_h(q, s, b).start()

    def products(q):
        gains = gain[:, chunk(q)]
        for b in range(ntp):
            part = lax.dot_general(vgx[b], wx[tfrom[b], chunk(q), :], nt, preferred_element_type=jnp.float32)
            gn[:, chunk(q)] = part if b == 0 else gn[:, chunk(q)] + part

        @pl.loop(0, n)
        def _(j):
            @pl.loop(0, Th // ROWS)
            def _(i):
                rows = span(j * T + c * Th + i * ROWS, ROWS, ROWS)
                here = span(j * Th + i * ROWS, ROWS, ROWS)
                t = gn[here, chunk(q)] * (cols[rows, chunk(q)].astype(jnp.float32) * spread(invc[rows, :]))
                gacc[:, chunk(q)] += jnp.sum(t.reshape(ROWS // 8, 8, Fc), axis=0)
                scaled = t * gains
                part = scaled[:, :LANES]
                for k in range(1, wide):
                    part = part + scaled[:, k * LANES:(k + 1) * LANES]
                rsc[here, :] += part

    def partial(q):
        gains = gain[:, chunk(q)]

        @pl.loop(0, n * T // ROWS)
        def _(i):
            rows = span(i * ROWS, ROWS, ROWS)
            normal = cols[rows, chunk(q)].astype(jnp.float32) * spread(invc[rows, :])
            nm[rows, chunk(q)] = (normal * gains).astype(jnp.bfloat16)

        wp[chunk(q), :] = lax.dot_general(nm[:, chunk(q)], vgs[...], tn, preferred_element_type=jnp.float32)

    A, B = factor(nrep)
    ra, rb = r // B, lax.rem(r, B)
    Fh = Fc // 2

    def axes(o):
        first = (rb, B, lambda i: {"rep": ra * B + i})
        second = (ra, A, lambda i: {"rep": i * B + rb})
        return (first, second) if o == 0 else (second, first)

    def rows1(q, o, i):
        size = Fh // axes(o)[0][1]
        return span(q * Fc + o * Fh + i * size, size, 8)

    def rows2(q, o, i):
        size = Fh // nrep
        return span(q * Fc + o * Fh + axes(o)[0][0] * (size * axes(o)[1][1]) + i * size, size, 8)

    def copy_p(stage, q, o, s):
        first, second = axes(o)
        mine_at, count, dev = (first, second, second, first)[stage]
        to = lax.rem(mine_at + s, count)
        if stage == 0:
            src, dst = wp.at[rows1(q, o, to)], wr1.at[q, o, s, :Fh // first[1]]
        elif stage == 1:
            size = Fh // nrep
            src, dst = ws1.at[q, o, span(to * size, size, 8)], wr2.at[q, o, s]
        elif stage == 2:
            src = dst = dw.at[rows2(q, o, mine_at)]
        else:
            src = dst = dw.at[rows1(q, o, mine_at)]
        at = (stage * C + q) * 2 + o
        return remote(src, dst, s_p.at[at, s], r_p.at[at, s], dev(to))

    def got_p(stage, q, o, s):
        first, second = axes(o)
        mine_at, count, dev = (first, second, second, first)[stage]
        source = lax.rem(mine_at + count - s, count)
        at = (stage * C + q) * 2 + o
        if stage == 0:
            ref = wr1.at[q, o, s, :Fh // first[1]]
        elif stage == 1:
            ref = wr2.at[q, o, s]
        elif stage == 2:
            ref = dw.at[rows2(q, o, source)]
        else:
            ref = dw.at[rows1(q, o, source)]
        return remote(ref, ref, s_p.at[at, s], r_p.at[at, s], dev(lax.rem(mine_at + s, count)))

    def counts(stage, o):
        first, second = axes(o)
        return (first, second, second, first)[stage][1]

    def stage_p(stage, q):
        for o in range(2):
            first, second = axes(o)
            if stage:
                for s in range(1, counts(stage - 1, o)):
                    got_p(stage - 1, q, o, s).wait_recv()
            if stage == 1:
                total = wp[rows1(q, o, first[0]), :]
                for s in range(1, first[1]):
                    total = total + wr1[q, o, s, :Fh // first[1]]
                ws1[q, o, :Fh // first[1]] = total
            elif stage == 2:
                size = Fh // nrep
                total = ws1[q, o, span(second[0] * size, size, 8)]
                for s in range(1, second[1]):
                    total = total + wr2[q, o, s]
                dw[rows2(q, o, second[0]), :] = total * average
            if stage < 4:
                for s in range(1, counts(stage, o)):
                    copy_p(stage, q, o, s).start()

    done = [0] * C

    def advance(steps):
        for q, upto in steps:
            while done[q] < min(upto, 5):
                stage_p(done[q], q)
                done[q] += 1

    def send_rs(s):
        return remote(rs.at[f], rs.at[f], s_rs.at[s], r_rs.at[s], {"fsdp": zpeer[s]})

    def got_rs(s):
        ref = rs.at[zfrom[s]]
        return remote(ref, ref, s_rs.at[s], r_rs.at[s], {"fsdp": zpeer[s]})

    for b in range(1, ntp):
        took_w(b).wait_recv()
        for j in range(n):
            pass_v(j, b).wait_recv()

    for q in range(C):
        arrive_h(q)
        if q == C - 1:
            products(q)
            for j in range(n):
                for k in range(Th // LANES):
                    block = rsc[span(j * Th + k * LANES, LANES), :].T
                    rs[f, j:j + 1, k * LANES:(k + 1) * LANES] = jnp.sum(block, axis=0, keepdims=True)
            for s in range(1, n):
                send_rs(s).start()
        for s in order:
            for b in range(1, ntp):
                took_h(q, s, b).wait_recv()
        partial(q)
        advance([(q, 1)])
        if q < C - 1:
            products(q)
            advance([(p, q - p + 1) for p in range(q)])

    slot = r * ntp + c
    gbuf[slot] = jnp.sum(gacc[...], axis=0, keepdims=True)

    def send_g(a, b):
        return remote(gbuf.at[slot], gbuf.at[slot], s_g.at[a, b], r_g.at[a, b], {"rep": rpeer[a], "tp": tpeer[b]})

    def got_g(a, b):
        ref = gbuf.at[lax.rem(r + nrep - a, nrep) * ntp + tfrom[b]]
        return remote(ref, ref, s_g.at[a, b], r_g.at[a, b], {"rep": rpeer[a], "tp": tpeer[b]})

    others = [(a, b) for a in range(nrep) for b in range(ntp) if a or b]
    for a, b in others:
        send_g(a, b).start()

    for s in range(1, n):
        got_rs(s).wait_recv()
    center = rs[0, :n, :]
    for s in range(1, n):
        center = center + rs[s, :n, :]
    cenc[:n, :] = center / D

    def send_b(s):
        return remote(cg.at[mine(zpeer[s])], dx.at[tokens(c), span(f * F, F)], s_b.at[s], r_b.at[s], {"fsdp": zpeer[s]})

    def got_b(s):
        ref = dx.at[tokens(c), span(zfrom[s] * F, F)]
        return remote(ref, ref, s_b.at[s], r_b.at[s], {"fsdp": zpeer[s]})

    def pass_b(s, b):
        ref = dx.at[tokens(c), span(zfrom[s] * F, F)]
        return remote(ref, ref, s_bx.at[b, s], r_bx.at[b, s], {"tp": tpeer[b]})

    def took_b(s, b):
        ref = dx.at[tokens(tfrom[b]), span(zfrom[s] * F, F)]
        return remote(ref, ref, s_bx.at[b, s], r_bx.at[b, s], {"tp": tpeer[b]})

    for s in [*order, 0]:
        j = zpeer[s]
        for k in range(Th // LANES):
            row = cenc[pl.ds(j, 1), k * LANES:(k + 1) * LANES]
            rsc[k * LANES:(k + 1) * LANES, :] = jnp.broadcast_to(row, (LANES, LANES)).T

        @pl.loop(0, Th // ROWS)
        def _(i):
            rows = span(j * T + c * Th + i * ROWS, ROWS, ROWS)
            here = span(j * Th + i * ROWS, ROWS, ROWS)
            inv, cen = invc[rows, :], rsc[span(i * ROWS, ROWS, ROWS), :]
            for q in range(C):
                scale = spread(inv)
                normal = cols[rows, chunk(q)].astype(jnp.float32) * scale
                cg[here, chunk(q)] = (scale * (gn[here, chunk(q)] * gain[:, chunk(q)] - normal * spread(cen))).astype(jnp.bfloat16)

        if s:
            send_b(s).start()
        else:
            dx[tokens(c), span(f * F, F)] = cg[mine(f), :]
            for b in range(1, ntp):
                pass_b(0, b).start()

    for stage in range(2, 6):
        advance([(q, max(done[q] + 1, stage)) for q in range(C)])
    for a, b in others:
        got_g(a, b).wait_recv()
    gsum = gbuf[0]
    for i in range(1, nrep * ntp):
        gsum = gsum + gbuf[i]
    dgain[...] = gsum * average

    for s in order:
        got_b(s).wait_recv()
        for b in range(1, ntp):
            pass_b(s, b).start()
    advance([(q, 5) for q in range(C)])
    for s in range(n):
        for b in range(1, ntp):
            took_b(s, b).wait_recv()
    for d in range(n):
        for right in (True, False):
            @pl.when(sends_v(d, right))
            def _():
                hop_v(d, right).wait_send()
    for s in range(1, n):
        for copy in (send_i(s), send_rs(s), send_b(s), *[send_h(q, s) for q in range(C)]):
            copy.wait_send()
    for q in range(C):
        for o in range(2):
            for stage in range(4):
                for s in range(1, counts(stage, o)):
                    copy_p(stage, q, o, s).wait_send()
    for a, b in others:
        send_g(a, b).wait_send()
    for b in range(1, ntp):
        pass_w(b).wait_send()
        for s in range(n):
            pass_v(s, b).wait_send()
            pass_b(s, b).wait_send()
            if s:
                for q in range(C):
                    pass_h(q, s, b).wait_send()


def store(*refs):
    sems = refs[-1]
    copies = [pltpu.make_async_copy(refs[i], refs[i + 3], sems.at[i]) for i in range(3)]
    for copy in copies:
        copy.start()
    for copy in copies:
        copy.wait()


def shards(hidden, norm_gain, value_weight, value_grad):
    nrep, n, ntp = (lax.axis_size(a) for a in ("rep", "fsdp", "tp"))
    T, D = hidden.shape
    F, K = value_weight.shape
    Th = T // ntp
    C = chunks_of(F)
    Fh = F // C // 2
    A, B = factor(nrep)
    G = n * T
    n8 = -(-n // 8) * 8
    dma = pltpu.SemaphoreType.DMA
    f32, bf16 = jnp.float32, jnp.bfloat16
    V = pltpu.VMEM
    vmem = pl.BlockSpec(memory_space=pltpu.VMEM)
    hbm = pl.BlockSpec(memory_space=pl.ANY)
    dx, dw, dgain = pl.pallas_call(
        functools.partial(kernel, (nrep, n, ntp)),
        out_shape=(V((T, D), bf16), V((F, K), f32), V((1, F), f32)),
        in_specs=[hbm, vmem, hbm, hbm],
        out_specs=(vmem, vmem, vmem),
        scratch_shapes=[
            V((T, D), bf16), V((G, F), bf16), V((G, F), bf16), V((G, K), bf16), V((ntp, n * Th, K), bf16),
            V((ntp, F, K), bf16), V((G, LANES), f32), V((n, 8, T), f32), V((n * Th, F), f32), V((n * Th, LANES), f32),
            V((n, n8, Th), f32), V((n8, Th), f32), V((n * Th, F), bf16), V((F, K), f32),
            V((C, 2, A, Fh // B, K), f32), V((C, 2, Fh // B, K), f32), V((C, 2, A, Fh // nrep, K), f32),
            V((8, F), f32), V((nrep * ntp, 1, F), f32),
            dma((3,)), dma((C, n)), dma((C, n)), dma((ntp, C * n)), dma((ntp, C * n)), dma((2, n)), dma((n,)),
            dma((ntp, n)), dma((ntp, n)), dma((ntp,)), dma((ntp,)), dma((n,)), dma((n,)),
            dma((n,)), dma((n,)), dma((n,)), dma((n,)), dma((ntp, n)), dma((ntp, n)),
            dma((8 * C, A)), dma((8 * C, A)), dma((nrep, ntp)), dma((nrep, ntp)),
        ],
        compiler_params=pltpu.CompilerParams(collective_id=0, has_side_effects=True, vmem_limit_bytes=59 * 1024 * 1024),
    )(hidden, norm_gain.reshape(1, F), value_weight, value_grad)
    dx, dw, dgain = pl.pallas_call(
        store,
        out_shape=tuple(jax.ShapeDtypeStruct(x.shape, x.dtype) for x in (dx, dw, dgain)),
        in_specs=[vmem] * 3,
        out_specs=(hbm,) * 3,
        scratch_shapes=[dma((3,))],
        compiler_params=pltpu.CompilerParams(vmem_limit_bytes=16 * 1024 * 1024),
    )(dx, dw, dgain)
    return dx, dw, dgain.reshape(F)


def solution(mesh):
    placed = (P(("rep", "fsdp"), None), P("fsdp"), P("fsdp", "tp"), P(("rep", "fsdp"), "tp"))
    return jax.shard_map(
        shards,
        mesh=mesh,
        in_specs=placed,
        out_specs=(P(("rep", "fsdp"), None), P("fsdp", "tp"), P("fsdp")),
        check_vma=False,
    )
```

```python
import functools

import jax
import jax.numpy as jnp
from jax import lax
from jax.experimental import pallas as pl
from jax.experimental.pallas import tpu as pltpu
from jax.sharding import PartitionSpec as P

epsilon = 1e-05
MESH = pl.DeviceIdType.MESH
ROWS = 32
LANES = 128


def factor(count):
    small = 1
    for d in range(1, count + 1):
        if count % d == 0 and d * d <= count:
            small = d
    return count // small, small


def chunks_of(F):
    for count in (4, 2):
        if F % (count * LANES) == 0:
            return count
    return 1


def kernel(sizes, hid, gain, w, vg, dx, dw, dgain,
           hv, cols, nm, vgs, vgx, wx, invc, inv_rows, gn, rsc, rs, cenc, cg, wp, wr1, ws1, wr2, gacc, gbuf,
           s_load, s_h, r_h, s_hx, r_hx, s_v, r_v, s_vx, r_vx, s_w, r_w, s_i, r_i,
           s_rs, r_rs, s_b, r_b, s_bx, r_bx, s_p, r_p, s_g, r_g):
    nrep, n, ntp = sizes
    r, f, c = lax.axis_index("rep"), lax.axis_index("fsdp"), lax.axis_index("tp")
    T, D = hid.shape
    F, K = w.shape
    Th = T // ntp
    C = chunks_of(F)
    Fc = F // C
    average = 1.0 / (nrep * n)
    wide = Fc // LANES
    nt = (((1,), (1,)), ((), ()))
    tn = (((0,), (0,)), ((), ()))

    def remote(src, dst, ssem, rsem, dev):
        return pltpu.make_async_remote_copy(src_ref=src, dst_ref=dst, send_sem=ssem, recv_sem=rsem,
                                            device_id=dev, device_id_type=MESH)

    def span(start, count, unit=LANES):
        return pl.ds(pl.multiple_of(start, unit), count)

    def half(j, h):
        return span(j * T + h * Th, Th)

    def full(j):
        return span(j * T, T)

    def tokens(h):
        return span(h * Th, Th)

    def mine(j):
        return span(j * Th, Th)

    def chunk(q):
        return slice(q * Fc, (q + 1) * Fc)

    zpeer = [lax.rem(f + s, n) for s in range(n)]
    zfrom = [lax.rem(f + n - s, n) for s in range(n)]
    tpeer = [lax.rem(c + s, ntp) for s in range(ntp)]
    tfrom = [lax.rem(c + ntp - s, ntp) for s in range(ntp)]
    rpeer = [lax.rem(r + s, nrep) for s in range(nrep)]

    load_h = pltpu.make_async_copy(hid, hv, s_load.at[0])
    load_v = pltpu.make_async_copy(vg, vgs.at[full(f)], s_load.at[1])
    load_w = pltpu.make_async_copy(w, wx.at[c], s_load.at[2])
    load_h.start()
    load_v.start()
    load_w.start()

    barrier = pltpu.get_barrier_semaphore()
    for s in range(1, n):
        pl.semaphore_signal(barrier, inc=1, device_id={"fsdp": zpeer[s]}, device_id_type=MESH)
    for a in range(nrep):
        for b in range(ntp):
            if a or b:
                pl.semaphore_signal(barrier, inc=1, device_id={"rep": rpeer[a], "tp": tpeer[b]}, device_id_type=MESH)
    pl.semaphore_wait(barrier, n - 1 + nrep * ntp - 1)

    def hop_v(d, right, p):
        j = f - d if right else f + d
        rows = span(j * T + p * (T // 2), T // 2)
        src = vg.at[p * (T // 2):(p + 1) * (T // 2)] if d == 0 else vgs.at[rows]
        return remote(src, vgs.at[rows], s_v.at[2 * int(right) + p, d], r_v.at[p, j], {"fsdp": f + 1 if right else f - 1})

    def has_v(d, right):
        return f - d >= 0 if right else f + d < n

    def sends_v(d, right):
        return jnp.logical_and(has_v(d, right), f + 1 < n if right else f >= 1)

    def pass_v(j, b, own=False):
        src = vg.at[tokens(tpeer[b])] if own else vgs.at[half(j, tpeer[b])]
        return remote(src, vgx.at[b, mine(j)], s_vx.at[b, j], r_vx.at[b, j], {"tp": tpeer[b]})

    def send_h(q, s):
        columns = span(zpeer[s] * F + q * Fc, Fc)
        return remote(hid.at[tokens(c), columns], cols.at[half(f, c), chunk(q)], s_h.at[q, s], r_h.at[q, s], {"fsdp": zpeer[s]})

    def got_h(q, s):
        ref = cols.at[half(zfrom[s], c), chunk(q)]
        return remote(ref, ref, s_h.at[q, s], r_h.at[q, s], {"fsdp": zpeer[s]})

    def pass_h(q, s, b):
        ref = cols.at[half(zfrom[s], c), chunk(q)]
        return remote(ref, ref, s_hx.at[b, q * n + s], r_hx.at[b, q * n + s], {"tp": tpeer[b]})

    def took_h(q, s, b):
        ref = cols.at[half(zfrom[s], tfrom[b]), chunk(q)]
        return remote(ref, ref, s_hx.at[b, q * n + s], r_hx.at[b, q * n + s], {"tp": tpeer[b]})

    def send_i(s):
        return remote(inv_rows.at[f], inv_rows.at[f], s_i.at[s], r_i.at[s], {"fsdp": zpeer[s]})

    def got_i(s):
        ref = inv_rows.at[zfrom[s]]
        return remote(ref, ref, s_i.at[s], r_i.at[s], {"fsdp": zpeer[s]})

    def pass_w(b):
        return remote(w, wx.at[c], s_w.at[b], r_w.at[b], {"tp": tpeer[b]})

    def took_w(b):
        ref = wx.at[tfrom[b]]
        return remote(ref, ref, s_w.at[b], r_w.at[b], {"tp": tpeer[b]})

    def arrive_v(d):
        for p in range(2):
            for right in (True, False):
                @pl.when(has_v(d, right))
                def _():
                    j = f - d if right else f + d
                    hop_v(d, right, p).wait_recv()
                    if p == 1:
                        for b in range(1, ntp):
                            pass_v(j, b).start()

                @pl.when(sends_v(d, right))
                def _():
                    hop_v(d, right, p).start()

    for p in range(2):
        for right in (True, False):
            @pl.when(sends_v(0, right))
            def _():
                hop_v(0, right, p).start()
    order = list(range(1, n))
    for s in order:
        send_h(0, s).start()
    for b in range(1, ntp):
        pass_w(b).start()
        pass_v(f, b, True).start()

    load_h.wait()

    @pl.loop(0, T // ROWS)
    def _(i):
        rows = span(i * ROWS, ROWS, ROWS)
        acc = jnp.zeros((ROWS, LANES), jnp.float32)
        for k in range(D // LANES):
            x = hv[rows, k * LANES:(k + 1) * LANES].astype(jnp.float32)
            acc = acc + x * x
        inv = lax.rsqrt(jnp.sum(acc, axis=1, keepdims=True) / D + epsilon)
        invc[span(f * T + i * ROWS, ROWS, ROWS), :] = jnp.broadcast_to(inv, (ROWS, LANES))

    for k in range(T // LANES):
        inv_rows[f, :, k * LANES:(k + 1) * LANES] = invc[span(f * T + k * LANES, LANES), :].T[:8, :]
    for s in range(1, n):
        send_i(s).start()
    for d in range(1, max(n, C)):
        if d < n:
            arrive_v(d)
        if d < C:
            for s in order:
                send_h(d, s).start()

    cols[full(f), :] = hv[:, span(f * F, F)]
    load_v.wait()
    load_w.wait()
    for j in range(n):
        vgx[0, mine(j), :] = vgs[half(j, c), :]
    for s in range(1, n):
        j = zfrom[s]
        got_i(s).wait_recv()
        for k in range(T // LANES):
            row = inv_rows[j, :1, k * LANES:(k + 1) * LANES]
            invc[span(j * T + k * LANES, LANES), :] = jnp.broadcast_to(row, (LANES, LANES)).T
    gacc[...] = jnp.zeros_like(gacc)
    rsc[...] = jnp.zeros_like(rsc)

    def spread(x, count=wide):
        return jnp.concatenate([x] * count, axis=1) if count > 1 else x

    def arrive_h(q):
        for s in order:
            got_h(q, s).wait_recv()
            for b in range(1, ntp):
                pass_h(q, s, b).start()

    def products(q):
        gains = gain[:, chunk(q)]
        for b in range(ntp):
            part = lax.dot_general(vgx[b], wx[tfrom[b], chunk(q), :], nt, preferred_element_type=jnp.float32)
            gn[:, chunk(q)] = part if b == 0 else gn[:, chunk(q)] + part

        @pl.loop(0, n)
        def _(j):
            @pl.loop(0, Th // ROWS)
            def _(i):
                rows = span(j * T + c * Th + i * ROWS, ROWS, ROWS)
                here = span(j * Th + i * ROWS, ROWS, ROWS)
                t = gn[here, chunk(q)] * (cols[rows, chunk(q)].astype(jnp.float32) * spread(invc[rows, :]))
                gacc[:, chunk(q)] += jnp.sum(t.reshape(ROWS // 8, 8, Fc), axis=0)
                scaled = t * gains
                part = scaled[:, :LANES]
                for k in range(1, wide):
                    part = part + scaled[:, k * LANES:(k + 1) * LANES]
                rsc[here, :] += part

    def partial(q):
        gains = gain[:, chunk(q)]

        @pl.loop(0, n * T // ROWS)
        def _(i):
            rows = span(i * ROWS, ROWS, ROWS)
            normal = cols[rows, chunk(q)].astype(jnp.float32) * spread(invc[rows, :])
            nm[rows, chunk(q)] = (normal * gains).astype(jnp.bfloat16)

        wp[chunk(q), :] = lax.dot_general(nm[:, chunk(q)], vgs[...], tn, preferred_element_type=jnp.float32)

    A, B = factor(nrep)
    ra, rb = r // B, lax.rem(r, B)
    Fh = Fc // 2

    def axes(o):
        first = (rb, B, lambda i: {"rep": ra * B + i})
        second = (ra, A, lambda i: {"rep": i * B + rb})
        return (first, second) if o == 0 else (second, first)

    def rows1(q, o, i):
        size = Fh // axes(o)[0][1]
        return span(q * Fc + o * Fh + i * size, size, 8)

    def rows2(q, o, i):
        size = Fh // nrep
        return span(q * Fc + o * Fh + axes(o)[0][0] * (size * axes(o)[1][1]) + i * size, size, 8)

    def copy_p(stage, q, o, s):
        first, second = axes(o)
        mine_at, count, dev = (first, second, second, first)[stage]
        to = lax.rem(mine_at + s, count)
        if stage == 0:
            src, dst = wp.at[rows1(q, o, to)], wr1.at[q, o, s, :Fh // first[1]]
        elif stage == 1:
            size = Fh // nrep
            src, dst = ws1.at[q, o, span(to * size, size, 8)], wr2.at[q, o, s]
        elif stage == 2:
            src = dst = dw.at[rows2(q, o, mine_at)]
        else:
            src = dst = dw.at[rows1(q, o, mine_at)]
        at = (stage * C + q) * 2 + o
        return remote(src, dst, s_p.at[at, s], r_p.at[at, s], dev(to))

    def got_p(stage, q, o, s):
        first, second = axes(o)
        mine_at, count, dev = (first, second, second, first)[stage]
        source = lax.rem(mine_at + count - s, count)
        at = (stage * C + q) * 2 + o
        if stage == 0:
            ref = wr1.at[q, o, s, :Fh // first[1]]
        elif stage == 1:
            ref = wr2.at[q, o, s]
        elif stage == 2:
            ref = dw.at[rows2(q, o, source)]
        else:
            ref = dw.at[rows1(q, o, source)]
        return remote(ref, ref, s_p.at[at, s], r_p.at[at, s], dev(lax.rem(mine_at + s, count)))

    def counts(stage, o):
        first, second = axes(o)
        return (first, second, second, first)[stage][1]

    def stage_p(stage, q):
        for o in range(2):
            first, second = axes(o)
            if stage:
                for s in range(1, counts(stage - 1, o)):
                    got_p(stage - 1, q, o, s).wait_recv()
            if stage == 1:
                total = wp[rows1(q, o, first[0]), :]
                for s in range(1, first[1]):
                    total = total + wr1[q, o, s, :Fh // first[1]]
                ws1[q, o, :Fh // first[1]] = total
            elif stage == 2:
                size = Fh // nrep
                total = ws1[q, o, span(second[0] * size, size, 8)]
                for s in range(1, second[1]):
                    total = total + wr2[q, o, s]
                dw[rows2(q, o, second[0]), :] = total * average
            if stage < 4:
                for s in range(1, counts(stage, o)):
                    copy_p(stage, q, o, s).start()

    done = [0] * C

    def advance(steps):
        for q, upto in steps:
            while done[q] < min(upto, 5):
                stage_p(done[q], q)
                done[q] += 1

    def send_rs(s):
        return remote(rs.at[f], rs.at[f], s_rs.at[s], r_rs.at[s], {"fsdp": zpeer[s]})

    def got_rs(s):
        ref = rs.at[zfrom[s]]
        return remote(ref, ref, s_rs.at[s], r_rs.at[s], {"fsdp": zpeer[s]})

    for b in range(1, ntp):
        took_w(b).wait_recv()
        for j in range(n):
            pass_v(j, b).wait_recv()

    for q in range(C):
        arrive_h(q)
        if q == C - 1:
            products(q)
            for j in range(n):
                for k in range(Th // LANES):
                    block = rsc[span(j * Th + k * LANES, LANES), :].T
                    rs[f, j:j + 1, k * LANES:(k + 1) * LANES] = jnp.sum(block, axis=0, keepdims=True)
            for s in range(1, n):
                send_rs(s).start()
        for s in order:
            for b in range(1, ntp):
                took_h(q, s, b).wait_recv()
        partial(q)
        advance([(q, 1)])
        if q < C - 1:
            products(q)
            advance([(p, q - p + 1) for p in range(q)])

    slot = r * ntp + c
    gbuf[slot] = jnp.sum(gacc[...], axis=0, keepdims=True)

    def send_g(a, b):
        return remote(gbuf.at[slot], gbuf.at[slot], s_g.at[a, b], r_g.at[a, b], {"rep": rpeer[a], "tp": tpeer[b]})

    def got_g(a, b):
        ref = gbuf.at[lax.rem(r + nrep - a, nrep) * ntp + tfrom[b]]
        return remote(ref, ref, s_g.at[a, b], r_g.at[a, b], {"rep": rpeer[a], "tp": tpeer[b]})

    others = [(a, b) for a in range(nrep) for b in range(ntp) if a or b]
    for a, b in others:
        send_g(a, b).start()

    for s in range(1, n):
        got_rs(s).wait_recv()
    center = rs[0, :n, :]
    for s in range(1, n):
        center = center + rs[s, :n, :]
    cenc[:n, :] = center / D

    def send_b(s):
        return remote(cg.at[mine(zpeer[s])], dx.at[tokens(c), span(f * F, F)], s_b.at[s], r_b.at[s], {"fsdp": zpeer[s]})

    def got_b(s):
        ref = dx.at[tokens(c), span(zfrom[s] * F, F)]
        return remote(ref, ref, s_b.at[s], r_b.at[s], {"fsdp": zpeer[s]})

    def pass_b(s, b):
        ref = dx.at[tokens(c), span(zfrom[s] * F, F)]
        return remote(ref, ref, s_bx.at[b, s], r_bx.at[b, s], {"tp": tpeer[b]})

    def took_b(s, b):
        ref = dx.at[tokens(tfrom[b]), span(zfrom[s] * F, F)]
        return remote(ref, ref, s_bx.at[b, s], r_bx.at[b, s], {"tp": tpeer[b]})

    for s in [*order, 0]:
        j = zpeer[s]
        for k in range(Th // LANES):
            row = cenc[pl.ds(j, 1), k * LANES:(k + 1) * LANES]
            rsc[k * LANES:(k + 1) * LANES, :] = jnp.broadcast_to(row, (LANES, LANES)).T

        @pl.loop(0, Th // ROWS)
        def _(i):
            rows = span(j * T + c * Th + i * ROWS, ROWS, ROWS)
            here = span(j * Th + i * ROWS, ROWS, ROWS)
            inv, cen = invc[rows, :], rsc[span(i * ROWS, ROWS, ROWS), :]
            for q in range(C):
                scale = spread(inv)
                normal = cols[rows, chunk(q)].astype(jnp.float32) * scale
                cg[here, chunk(q)] = (scale * (gn[here, chunk(q)] * gain[:, chunk(q)] - normal * spread(cen))).astype(jnp.bfloat16)

        if s:
            send_b(s).start()
        else:
            dx[tokens(c), span(f * F, F)] = cg[mine(f), :]
            for b in range(1, ntp):
                pass_b(0, b).start()

    for stage in range(2, 6):
        advance([(q, max(done[q] + 1, stage)) for q in range(C)])
    for a, b in others:
        got_g(a, b).wait_recv()
    gsum = gbuf[0]
    for i in range(1, nrep * ntp):
        gsum = gsum + gbuf[i]
    dgain[...] = gsum * average

    for s in order:
        got_b(s).wait_recv()
        for b in range(1, ntp):
            pass_b(s, b).start()
    advance([(q, 5) for q in range(C)])
    for s in range(n):
        for b in range(1, ntp):
            took_b(s, b).wait_recv()
    for d in range(n):
        for right in (True, False):
            @pl.when(sends_v(d, right))
            def _():
                hop_v(d, right, 0).wait_send()
                hop_v(d, right, 1).wait_send()
    for s in range(1, n):
        for copy in (send_i(s), send_rs(s), send_b(s), *[send_h(q, s) for q in range(C)]):
            copy.wait_send()
    for q in range(C):
        for o in range(2):
            for stage in range(4):
                for s in range(1, counts(stage, o)):
                    copy_p(stage, q, o, s).wait_send()
    for a, b in others:
        send_g(a, b).wait_send()
    for b in range(1, ntp):
        pass_w(b).wait_send()
        for s in range(n):
            pass_v(s, b).wait_send()
            pass_b(s, b).wait_send()
            if s:
                for q in range(C):
                    pass_h(q, s, b).wait_send()


def store(*refs):
    sems = refs[-1]
    copies = [pltpu.make_async_copy(refs[i], refs[i + 3], sems.at[i]) for i in range(3)]
    for copy in copies:
        copy.start()
    for copy in copies:
        copy.wait()


def shards(hidden, norm_gain, value_weight, value_grad):
    nrep, n, ntp = (lax.axis_size(a) for a in ("rep", "fsdp", "tp"))
    T, D = hidden.shape
    F, K = value_weight.shape
    Th = T // ntp
    C = chunks_of(F)
    Fh = F // C // 2
    A, B = factor(nrep)
    G = n * T
    n8 = -(-n // 8) * 8
    dma = pltpu.SemaphoreType.DMA
    f32, bf16 = jnp.float32, jnp.bfloat16
    V = pltpu.VMEM
    vmem = pl.BlockSpec(memory_space=pltpu.VMEM)
    hbm = pl.BlockSpec(memory_space=pl.ANY)
    dx, dw, dgain = pl.pallas_call(
        functools.partial(kernel, (nrep, n, ntp)),
        out_shape=(V((T, D), bf16), V((F, K), f32), V((1, F), f32)),
        in_specs=[hbm, vmem, hbm, hbm],
        out_specs=(vmem, vmem, vmem),
        scratch_shapes=[
            V((T, D), bf16), V((G, F), bf16), V((G, F), bf16), V((G, K), bf16), V((ntp, n * Th, K), bf16),
            V((ntp, F, K), bf16), V((G, LANES), f32), V((n, 8, T), f32), V((n * Th, F), f32), V((n * Th, LANES), f32),
            V((n, n8, Th), f32), V((n8, Th), f32), V((n * Th, F), bf16), V((F, K), f32),
            V((C, 2, A, Fh // B, K), f32), V((C, 2, Fh // B, K), f32), V((C, 2, A, Fh // nrep, K), f32),
            V((8, F), f32), V((nrep * ntp, 1, F), f32),
            dma((3,)), dma((C, n)), dma((C, n)), dma((ntp, C * n)), dma((ntp, C * n)), dma((4, n)), dma((2, n)),
            dma((ntp, n)), dma((ntp, n)), dma((ntp,)), dma((ntp,)), dma((n,)), dma((n,)),
            dma((n,)), dma((n,)), dma((n,)), dma((n,)), dma((ntp, n)), dma((ntp, n)),
            dma((8 * C, A)), dma((8 * C, A)), dma((nrep, ntp)), dma((nrep, ntp)),
        ],
        compiler_params=pltpu.CompilerParams(collective_id=0, has_side_effects=True, vmem_limit_bytes=59 * 1024 * 1024),
    )(hidden, norm_gain.reshape(1, F), value_weight, value_grad)
    dx, dw, dgain = pl.pallas_call(
        store,
        out_shape=tuple(jax.ShapeDtypeStruct(x.shape, x.dtype) for x in (dx, dw, dgain)),
        in_specs=[vmem] * 3,
        out_specs=(hbm,) * 3,
        scratch_shapes=[dma((3,))],
        compiler_params=pltpu.CompilerParams(vmem_limit_bytes=16 * 1024 * 1024),
    )(dx, dw, dgain)
    return dx, dw, dgain.reshape(F)


def solution(mesh):
    placed = (P(("rep", "fsdp"), None), P("fsdp"), P("fsdp", "tp"), P(("rep", "fsdp"), "tp"))
    return jax.shard_map(
        shards,
        mesh=mesh,
        in_specs=placed,
        out_specs=(P(("rep", "fsdp"), None), P("fsdp", "tp"), P("fsdp")),
        check_vma=False,
    )
```
